32 devices in a mesh: region: 8 (over z, x), member: 4 (over y, core).
Axes of the slice: x: 2, y: 2, z: 4, core: 2. Of those that a mesh axis runs over, the one named last changes fastest.
Arguments:
- members: float32 [256, 128, 1024], P('member', 'region'), may hold values from -6 to 6
- obs_value: float32 [128, 1024], P('region'), may hold values from -6 to 6
- obs_precision: float32 [128, 1024], P('region'), may hold values from 0.02 to 200
- obs_index: int32 [128, 1024], P('region'), may hold values from 0 to 1023, as said below
- obs_count: int32 [128], P('region'), may hold values from 256 to 1024
Outputs:
- analysis: float32 [256, 128, 1024], P('member', 'region')
The draws below stay inside these ranges and needn't reach their ends.
Inputs may be any that keep to these rules, and one draw needn't show every extreme that they name: `obs_count`: slots of a tile from its count onward are empty. `obs_index`: position within its own tile.
All inputs are finite; a program needn't handle non-finite values.
Results may differ from the reference program's by a relative error of at most 0.0005.
Values sent between devices are 32-bit elements; how exact they have to be, the bound alone decides.
A program may use at most 64 MiB of HBM per device.

```python
import math
import jax
import jax.numpy as jnp
from jax import lax

K = 256
TILE = 1024
OBS = 1024
TILES_DEV = 16
ITERS = 12
TILES = 128
N_REGION = 8


def draw_obs_index(key, part):
    hot_key = jax.random.fold_in(key, 11)
    pick_key = jax.random.fold_in(key, 12)
    wide_key = jax.random.fold_in(key, 13)
    centres = jax.random.randint(hot_key, (TILES, 4), 0, TILE, dtype=jnp.int32)
    selector = jax.random.randint(pick_key, (TILES, OBS), 0, 4, dtype=jnp.int32)
    spread = jax.random.randint(wide_key, (TILES, OBS), 0, TILE, dtype=jnp.int32)
    repeated = jnp.take_along_axis(centres, selector, axis=1)
    slot_ids = jnp.arange(OBS, dtype=jnp.int32)[None, :]
    return jnp.where(slot_ids < OBS // 8, repeated, spread).astype(jnp.int32)


def draw_obs_precision(key, part):
    low_key = jax.random.fold_in(key, 21)
    high_key = jax.random.fold_in(key, 22)
    background = jnp.exp(jax.random.uniform(low_key, (TILES, OBS), jnp.float32, math.log(0.02), math.log(2.0)))
    background = jnp.clip(background, 0.02, 2.0)
    precise = jnp.exp(jax.random.uniform(high_key, (TILES, OBS), jnp.float32, math.log(40.0), math.log(200.0)))
    precise = jnp.clip(precise, 40.0, 200.0)
    slot_ids = jnp.arange(OBS, dtype=jnp.int32)[None, :]
    return jnp.where(slot_ids < OBS // 8, precise, background).astype(jnp.float32)


def place_ends(values, stream_key, low, largest):
    spot = [jax.random.randint(jax.random.fold_in(stream_key, axis), (), 0, length) for axis, length in enumerate(values.shape)]
    main_axis = values.shape.index(max(values.shape))
    beside = spot[:main_axis] + [(spot[main_axis] + 1) % values.shape[main_axis]] + spot[main_axis + 1:]
    return values.at[tuple(spot)].set(low).at[tuple(beside)].set(largest)


def block_scale(key, shape, cuts, smallest, largest):
    loudness, own = 1.0, jax.random.fold_in(key, 6)
    for dim, shards_of in cuts:
        draws = jnp.exp(jax.random.uniform(jax.random.fold_in(own, dim), (shards_of,), jnp.float32, smallest / len(cuts), largest / len(cuts)))
        loudness = loudness * jnp.repeat(draws, shape[dim] // shards_of).reshape([-1 if axis == dim else 1 for axis in range(len(shape))])
    return loudness


def gaussian(key, dims, scale, most, cuts=(), held_as=jnp.bfloat16):
    values = scale * jax.random.normal(key, dims, jnp.float32)
    if cuts:
        values = values * block_scale(key, dims, cuts, -0.22, 0.18)
    return jnp.clip(values, -most, most).astype(held_as)


def setup_inputs(seed: int = 0) -> dict:
    keys = jax.random.split(jax.random.key(seed), 6)
    members = gaussian(keys[0], (K, TILES, TILE), 1.0, 6.0, ((0, 4), (1, 8)), jnp.float32)
    obs_value = gaussian(keys[1], (TILES, OBS), 1.0, 6.0, ((0, 8),), jnp.float32)
    obs_precision = draw_obs_precision(jax.random.fold_in(keys[5], 71), 0)
    obs_index = draw_obs_index(jax.random.fold_in(keys[5], 71), 0)
    obs_count = place_ends(jax.random.randint(keys[4], (TILES,), OBS // 4, OBS + 1), jax.random.fold_in(keys[4], 1), OBS // 4, OBS).astype(jnp.int32)
    return dict(members=members, obs_value=obs_value, obs_precision=obs_precision, obs_index=obs_index, obs_count=obs_count)


def observe(states, places, observed, accuracy, filled):
    average = lax.optimization_barrier(jnp.sum(states, axis=0)) / K
    deviation = states - average[None]
    sampled = jnp.take_along_axis(deviation, places[None], axis=2)
    baseline = jnp.take_along_axis(average, places, axis=1)
    slot_ids = jnp.arange(places.shape[1], dtype=jnp.int32)
    active = slot_ids[None, :] < filled[:, None]
    weight_root = jnp.where(active, jnp.sqrt(accuracy), jnp.float32(0.0))
    scaled = sampled * weight_root[None]
    innov_row = (weight_root * (observed - baseline))[None]
    stacked = jnp.concatenate([scaled, innov_row], axis=0)
    return (average, deviation, stacked)

def outer_gram(stacked):
    return jnp.einsum('ibo,jbo->bij', stacked, stacked, precision=lax.Precision.HIGHEST)

def transform_weights(gram_matrix):
    ensemble = gram_matrix.shape[1] - 1
    identity = jnp.eye(ensemble, dtype=jnp.float32)
    system = (ensemble - 1.0) * identity + gram_matrix[:, :ensemble, :ensemble]
    right_side = gram_matrix[:, :ensemble, ensemble]
    factor = jnp.sqrt(lax.optimization_barrier(jnp.sum(system * system, axis=(1, 2))) + 1e-06)
    root_iter = system / factor[:, None, None]
    inverse_iter = jnp.broadcast_to(identity, system.shape)

    def one_sweep(sweep_no, iterates):
        root_now, inverse_now = iterates
        middle = 3.0 * identity - jnp.einsum('bij,bjk->bik', inverse_now, root_now, precision=lax.Precision.HIGHEST)
        root_next = 0.5 * jnp.einsum('bij,bjk->bik', root_now, middle, precision=lax.Precision.HIGHEST)
        inverse_next = 0.5 * jnp.einsum('bij,bjk->bik', middle, inverse_now, precision=lax.Precision.HIGHEST)
        return (root_next, inverse_next)
    root_iter, inverse_iter = lax.fori_loop(0, ITERS, one_sweep, (root_iter, inverse_iter))
    inverse_root = inverse_iter / jnp.sqrt(factor)[:, None, None]
    pulled = jnp.einsum('bij,bj->bi', inverse_root, right_side, precision=lax.Precision.HIGHEST)
    shifted = jnp.einsum('bij,bj->bi', inverse_root, pulled, precision=lax.Precision.HIGHEST)
    return math.sqrt(ensemble - 1.0) * inverse_root + shifted[:, :, None]

def analyse(average, deviation, gram_matrix):
    weights = transform_weights(gram_matrix)
    return average[None] + jnp.einsum('jbc,bjk->kbc', deviation, weights, precision=lax.Precision.HIGHEST)

def reference(members, obs_value, obs_precision, obs_index, obs_count):
    columns = members.reshape(K, N_REGION, TILES_DEV, TILE).transpose(1, 0, 2, 3)
    obs_values = obs_value.reshape(N_REGION, TILES_DEV, OBS)
    accuracies = obs_precision.reshape(N_REGION, TILES_DEV, OBS)
    indices = obs_index.reshape(N_REGION, TILES_DEV, OBS)
    obs_counts = obs_count.reshape(N_REGION, TILES_DEV)

    def gram_of(entries):
        states, places, observed, accuracy, filled = entries
        return outer_gram(observe(states, places, observed, accuracy, filled)[2])
    gram_tiles = lax.map(gram_of, (columns, indices, obs_values, accuracies, obs_counts))
    combined = gram_tiles + 0.5 * (jnp.roll(gram_tiles, 1, axis=0) + jnp.roll(gram_tiles, -1, axis=0))

    def analyse_column(entries):
        states, places, observed, accuracy, filled, gram_matrix = entries
        average, deviation, stacked = observe(states, places, observed, accuracy, filled)
        return analyse(average, deviation, gram_matrix)
    result = lax.map(analyse_column, (columns, indices, obs_values, accuracies, obs_counts, combined))
    return result.transpose(1, 0, 2, 3).reshape(K, N_REGION * TILES_DEV, TILE)
```

```python
import functools
import math

import jax
import jax.numpy as jnp
from jax import lax
from jax.experimental import pallas as pl
from jax.experimental.pallas import tpu as pltpu
from jax.sharding import PartitionSpec as P

ITERS = 12
LANES = 128
F32 = jnp.float32
BF16 = jnp.bfloat16


def split3(x):
    a = x.astype(BF16)
    rest = x - a.astype(F32)
    b = rest.astype(BF16)
    return a, b, (rest - b.astype(F32)).astype(BF16)


def dot(a, b):
    return jnp.dot(a, b, preferred_element_type=F32)


def dot_nt(a, b):
    return lax.dot_general(a, b, (((1,), (1,)), ((), ())), preferred_element_type=F32)


def product(a, b):
    a1, a2, a3 = a
    b1, b2, b3 = b
    left = jnp.concatenate([a1, a3, a2, a1, a2, a1], axis=1)
    right = jnp.concatenate([b3, b1, b2, b2, b1, b1], axis=0)
    return dot(left, right)


def gram_kernel(x_ref, index_ref, value_ref, precision_ref, out_ref):
    states = x_ref[0]
    size, width = states.shape
    half = size // 2
    groups = width // LANES
    places, exact = index_ref[0], precision_ref[0]
    slots = places.shape[1]

    high = lax.shift_right_logical(places, 7)
    low = lax.bitwise_and(places, LANES - 1)
    rows = lax.broadcasted_iota(jnp.int32, (groups, slots), 0) == high
    both = jnp.concatenate(
        [jnp.where(rows, exact, 0.0), jnp.where(rows, exact * value_ref[0], 0.0)], axis=0
    )
    one_hot = jnp.where(
        lax.broadcasted_iota(jnp.int32, (LANES, slots), 0) == low, 1.0, 0.0
    ).astype(BF16)
    e1, e2, e3 = split3(both)
    sums = dot_nt(e3, one_hot) + dot_nt(e2, one_hot) + dot_nt(e1, one_hot)
    c = jnp.concatenate([sums[i : i + 1] for i in range(groups)], axis=1)
    d = jnp.concatenate([sums[groups + i : groups + i + 1] for i in range(groups)], axis=1)

    average = jnp.sum(states, axis=0, keepdims=True) / size
    deviation = states - average
    s1, s2, s3 = split3(deviation * jnp.sqrt(c))
    cross = dot_nt(s1, s3) + dot_nt(s1, s2)
    own = (dot_nt(s2, s2) + (cross + cross.T)) + dot_nt(s1, s1)

    pulled = deviation * (d - c * average)
    folded = pulled[:, :LANES]
    for i in range(1, groups):
        folded = folded + pulled[:, i * LANES : (i + 1) * LANES]
    right = jnp.sum(folded.T, axis=0, keepdims=True)

    row = lax.broadcasted_iota(jnp.int32, (half, half), 0)
    col = lax.broadcasted_iota(jnp.int32, (half, half), 1)
    first, last = own[:half, :half], own[half:, half:]
    diagonal = jnp.sum(jnp.where(row == col, last, 0.0), axis=0, keepdims=True)
    out_ref[0, :half, :half] = own[:half, half:]
    out_ref[0, :half, half:] = jnp.where(row <= col, first, last)
    tail = jnp.concatenate([right, jnp.concatenate([diagonal, diagonal], axis=1)], axis=0)
    out_ref[0, half:, :] = jnp.concatenate([tail, jnp.zeros((6, size), F32)], axis=0)


def analysis_kernel(own_ref, west_ref, east_ref, x_ref, out_ref, u_ref, z_ref):
    tiles, size, width = x_ref.shape
    half = size // 2
    row = lax.broadcasted_iota(jnp.int32, (size, size), 0)
    col = lax.broadcasted_iota(jnp.int32, (size, size), 1)
    identity = jnp.where(row == col, 1.0, 0.0).astype(F32)
    small_row, small_col = row[:half, :half], col[:half, :half]
    rights, scales = [], []

    def growth(u, z):
        x = split3(u if z is None else product(z, u))
        plain = u if z is None else x[0].astype(F32) + x[1].astype(F32) + x[2].astype(F32)
        squared = product(x, x)
        inner = (1 / 16) * squared - (9 / 16) * plain
        outer = product(split3(squared), split3(inner))
        return (36 / 16) * identity - (39 / 16) * plain + (27 / 16) * squared + outer

    for t in range(tiles):
        packed = own_ref[t] + 0.5 * (west_ref[t] + east_ref[t])
        upper, mixed = packed[:half, :half], packed[:half, half:]
        rights.append(packed[half : half + 1])
        diagonal = packed[half + 1 : half + 2, :half]
        turned = mixed.T
        first = jnp.where(small_row <= small_col, mixed, turned)
        last = jnp.where(small_row > small_col, mixed, turned)
        last = jnp.where(small_row == small_col, diagonal, last)
        gram = jnp.concatenate(
            [
                jnp.concatenate([first, upper], axis=1),
                jnp.concatenate([upper.T, last], axis=1),
            ],
            axis=0,
        )
        system = (size - 1.0) * identity + gram
        total = jnp.sum(jnp.sum(system * system, axis=0, keepdims=True), axis=1, keepdims=True)
        scale = jnp.sqrt(total + 1e-6)
        scales.append(scale)
        u = system / scale
        g = growth(u, None)
        z_ref[t] = g
        u_ref[t] = product(split3(u), split3(g))

    def two_steps(_, carry):
        for t in range(tiles):
            u, z = split3(u_ref[t]), split3(z_ref[t])
            g = split3(growth(u, z))
            u_ref[t] = product(u, g)
            z_ref[t] = product(g, z)
        return carry

    lax.fori_loop(0, ITERS // 2 - 2, two_steps, 0)

    for t in range(tiles):
        u, z = split3(u_ref[t]), split3(z_ref[t])
        inverse = product(split3(growth(u, z)), z) / jnp.sqrt(scales[t])
        pulled = jnp.sum(inverse * rights[t], axis=1, keepdims=True)
        shift = jnp.sum(inverse * pulled, axis=0, keepdims=True)
        weights = math.sqrt(size - 1.0) * inverse + shift
        average = jnp.sum(x_ref[t], axis=0, keepdims=True) / size
        w1, w2, _ = split3(weights)
        d1, d2, _ = split3(x_ref[t] - average)
        left = jnp.concatenate([w2, w1, w1], axis=1)
        right = jnp.concatenate([d1, d2, d1], axis=0)
        out_ref[t] = average + dot(left, right)


def block(*shape):
    return pl.BlockSpec(shape, lambda i: (i,) + (0,) * (len(shape) - 1))


def grams(states, places, observed, accuracy):
    owned, size, width = states.shape
    slots = places.shape[1]
    table = block(1, 1, slots)
    return pl.pallas_call(
        gram_kernel,
        grid=(owned,),
        in_specs=[block(1, size, width), table, table, table],
        out_specs=block(1, size // 2 + 8, size),
        out_shape=jax.ShapeDtypeStruct((owned, size // 2 + 8, size), F32),
        cost_estimate=pl.CostEstimate(
            flops=owned * 12 * size * size * width, bytes_accessed=states.size * 4, transcendentals=0
        ),
    )(states, places[:, None], observed[:, None], accuracy[:, None])


def analyses(own, west, east, states):
    owned, size, width = states.shape
    tiles = 2 if owned % 2 == 0 else 1
    packed = block(tiles, size // 2 + 8, size)
    return pl.pallas_call(
        analysis_kernel,
        grid=(owned // tiles,),
        in_specs=[packed, packed, packed, block(tiles, size, width)],
        out_specs=block(tiles, size, width),
        out_shape=jax.ShapeDtypeStruct(states.shape, F32),
        scratch_shapes=[pltpu.VMEM((tiles, size, size), F32)] * 2,
        cost_estimate=pl.CostEstimate(
            flops=owned * 27 * 12 * size**3, bytes_accessed=states.size * 8, transcendentals=0
        ),
        compiler_params=pltpu.CompilerParams(vmem_limit_bytes=56 * 2**20),
    )(own, west, east, states)


def shards(chunks, members, obs_value, obs_precision, obs_index, obs_count):
    owned = members.shape[1] // lax.axis_size("member")
    parts = chunks if owned % chunks == 0 else 1
    first_band = lax.axis_index("member") * owned
    per = owned // parts
    count = lax.axis_size("member")
    rows, tiles, width = members.shape

    def own_rows(tables):
        return lax.dynamic_slice_in_dim(tables, first_band, owned, 0)

    filled = own_rows(obs_count)
    slot_ids = jnp.arange(obs_value.shape[1], dtype=jnp.int32)
    accuracy = jnp.where(slot_ids[None] < filled[:, None], own_rows(obs_precision), 0.0)
    places, observed = own_rows(obs_index), own_rows(obs_value)

    turned = members.reshape(rows, count, parts, per, width).transpose(2, 1, 3, 0, 4)
    columns = lax.axis_size("region")
    forward = [(i, (i + 1) % columns) for i in range(columns)]
    backward = [(b, a) for a, b in forward]
    gathered, packed = [], []
    for i in range(parts):
        got = lax.all_to_all(turned[i], "member", split_axis=0, concat_axis=0, tiled=False)
        got = got.transpose(1, 0, 2, 3).reshape(per, count * rows, width)
        span = slice(i * per, (i + 1) * per)
        own = grams(got, places[span], observed[span], accuracy[span])
        gathered.append(got)
        packed.append(
            (own, lax.ppermute(own, "region", forward), lax.ppermute(own, "region", backward))
        )
    results = []
    for i in range(parts):
        result = analyses(*packed[i], gathered[i])
        result = result.reshape(per, count, rows, width).transpose(1, 0, 2, 3)
        results.append(lax.all_to_all(result, "member", split_axis=0, concat_axis=0, tiled=False))
    return jnp.stack(results, axis=1).reshape(tiles, rows, width).transpose(1, 0, 2)


def solution(mesh):
    in_specs = (
        P("member", "region", None),
        P("region", None),
        P("region", None),
        P("region", None),
        P("region"),
    )
    out_specs = P("member", "region", None)
    return jax.shard_map(
        functools.partial(shards, 1),
        mesh=mesh,
        in_specs=in_specs,
        out_specs=out_specs,
        check_vma=False,
    )
```
